32 devices in a mesh: expert: 2 (over x), batch: 4 (over z), seq: 4 (over y, core).
Axes of the slice: x: 2, y: 2, z: 4, core: 2. Of those that a mesh axis runs over, the one named last changes fastest.
Arguments:
- queries: bfloat16 [2, 4, 2, 384, 4096], P('expert', 'batch', None, 'seq'), may hold values from -36 to 36
- keys: bfloat16 [2, 4, 2, 384, 4096], P('expert', 'batch', None, 'seq'), may hold values from -21 to 21
- values: bfloat16 [2, 4, 2, 384, 4096], P('expert', 'batch', None, 'seq'), may hold values from -6 to 6
- latents: bfloat16 [2, 4, 384, 4096], P('expert', 'batch', 'seq'), may hold values from -6 to 6
- gain: bfloat16 [2, 4096], P('expert'), may hold values from 0.099609375 to 1.8984375
- steps_table: int32 [2, 4], P('expert', 'batch'), may hold values from 0 to 38
- flags: int32 [4], P('batch'), may hold values 0 or 1
Outputs:
- denoised: bfloat16 [2, 4, 384, 4096], P('expert', 'batch', 'seq')
- next_latents: bfloat16 [2, 4, 384, 4096], P('expert', 'batch', 'seq')
The draws below stay inside these ranges and needn't reach their ends.
All inputs are finite; a program needn't handle non-finite values. No bound on the sum of `flags` on one device may be relied on, other than what follows from the above.
Results may differ from the reference program's by a relative error of at most 0.006.
Values may be sent and summed in bfloat16 or wider, within the bound.
A program may use at most 64 MiB of HBM per device.

```python
import jax
import jax.numpy as jnp
from jax import lax

HEADS = 32
HDIM = 128
STEPS = 40
BOUNDARY = 15
BATCH = 4
SEQ = 384
WIDTH = 4096


def paired_draw(key):
    base = jax.random.fold_in(key, 7)
    query_key, key_key = jax.random.split(base, 2)
    shape = (2, BATCH, 2, SEQ, HEADS * HDIM)
    query_part = jnp.clip(jax.random.normal(query_key, shape, jnp.float32), -5.0, 5.0)
    key_part = jnp.clip(jax.random.normal(key_key, shape, jnp.float32), -5.0, 5.0)
    return (query_part, key_part)


def draw_queries(key, part):
    return paired_draw(key)[0].astype(jnp.bfloat16)


def draw_keys(key, part):
    return paired_draw(key)[1].astype(jnp.bfloat16)


def draw_steps_table(key, part):
    base = jax.random.fold_in(key, 11)
    high_key, low_key, high_pick, low_pick = jax.random.split(base, 4)
    high_steps = jax.random.randint(high_key, (BATCH,), 0, BOUNDARY)
    low_steps = jax.random.randint(low_key, (BATCH,), BOUNDARY, STEPS - 1)
    places = jnp.arange(BATCH, dtype=jnp.int32)
    high_spot = jax.random.randint(high_pick, (), 0, BATCH)
    low_spot = jax.random.randint(low_pick, (), 0, BATCH)
    high_steps = jnp.where(places == high_spot, 0, high_steps)
    low_steps = jnp.where(places == low_spot, STEPS - 2, low_steps)
    return jnp.stack([high_steps, low_steps], axis=0).astype(jnp.int32)


def touch_ends(values, stream_key, low, largest):
    longest = values.shape.index(max(values.shape))
    spots = []
    for shift in (0, 1):
        where = [jax.random.randint(jax.random.fold_in(stream_key, axis), (), 0, length) for axis, length in enumerate(values.shape)]
        where[longest] = (where[longest] + shift) % values.shape[longest]
        spots.append(tuple(where))
    return values.at[spots[0]].set(low).at[spots[1]].set(largest)


def levels(stream_key, extent, shards, least, high):
    level, own = 1.0, jax.random.fold_in(stream_key, 6)
    for axis_at, parts in shards:
        heights = jnp.exp(jax.random.uniform(jax.random.fold_in(own, axis_at), (parts,), jnp.float32, least / len(shards), high / len(shards)))
        level = level * jnp.repeat(heights, extent[axis_at] // parts).reshape([-1 if axis == axis_at else 1 for axis in range(len(extent))])
    return level


def gaussian(rng, extent, scale, most, cuts=(), kind=jnp.bfloat16):
    result = scale * jax.random.normal(rng, extent, jnp.float32)
    if cuts:
        result = result * levels(rng, extent, cuts, -0.22, 0.18)
    return jnp.clip(result, -most, most).astype(kind)


def setup_inputs(seed: int = 0) -> dict:
    seeds = jax.random.split(jax.random.key(seed), 8)
    queries = draw_queries(jax.random.fold_in(seeds[7], 71), 0)
    keys = draw_keys(jax.random.fold_in(seeds[7], 71), 0)
    values = gaussian(seeds[2], (2, BATCH, 2, SEQ, WIDTH), 1.0, 6.0, ((0, 2), (1, 4), (3, 4)))
    latents = gaussian(seeds[3], (2, BATCH, SEQ, WIDTH), 1.0, 6.0, ((0, 2), (1, 4), (2, 4)))
    gain = jnp.clip(1.0 + 0.18 * jax.random.normal(seeds[4], (2, WIDTH), jnp.float32), 0.099609375, 1.8984375).astype(jnp.bfloat16)
    steps_table = draw_steps_table(jax.random.fold_in(seeds[7], 71), 0)
    flags = touch_ends((jax.random.randint(seeds[6], (BATCH,), 0, 2) < 1).astype(jnp.int32), jax.random.fold_in(seeds[6], 1), 0, 1)
    return dict(queries=queries, keys=keys, values=values, latents=latents, gain=gain, steps_table=steps_table, flags=flags)


GUIDANCE = 3.5
flow_shift = 5.0

def sigma_of(step):
    level = 1.0 - step.astype(jnp.float32) / STEPS
    return flow_shift * level / (1.0 + (flow_shift - 1.0) * level)

def attend_head(query, key_rows, value_rows):
    scores = jnp.dot(query, key_rows.T, preferred_element_type=jnp.float32) * HDIM ** (-0.5)
    weights = jax.nn.softmax(scores, axis=-1).astype(jnp.bfloat16)
    return jnp.dot(weights, value_rows, preferred_element_type=jnp.float32).astype(jnp.bfloat16)

def combine(cond, uncond):
    base = uncond.astype(jnp.float32)
    return (base + GUIDANCE * (cond.astype(jnp.float32) - base)).astype(jnp.bfloat16)

def reference(queries, keys, values, latents, gain, steps_table, flags):
    groups, clips, branches, length, width = queries.shape

    def heads_first(array):
        shaped = array.reshape(groups * clips * branches, length, HEADS, HDIM)
        return shaped.transpose(0, 2, 1, 3).reshape(-1, length, HDIM)
    outcome = lax.map(lambda triple: attend_head(*triple), (heads_first(queries), heads_first(keys), heads_first(values)))
    attended = outcome.reshape(groups, clips, branches, HEADS, length, HDIM)
    attended = attended.transpose(0, 1, 2, 4, 3, 5).reshape(groups, clips, branches, length, width)
    guided = combine(attended[:, :, 0], attended[:, :, 1]).astype(jnp.float32)
    scale = lax.rsqrt(lax.optimization_barrier(jnp.mean(guided * guided, axis=-1, keepdims=True)) + 1e-06)
    velocity = guided * scale * gain.astype(jnp.float32)[:, None, None, :]
    sigma_now = sigma_of(steps_table)[:, :, None, None]
    sigma_next = sigma_of(steps_table + 1)[:, :, None, None]
    current = latents.astype(jnp.float32)
    denoised = (current - sigma_now * velocity).astype(jnp.bfloat16)
    moved = (current + (sigma_next - sigma_now) * velocity).astype(jnp.bfloat16)
    crossing = (flags == 1)[None, :, None, None]
    next_latents = jnp.where(crossing, moved[::-1], moved)
    return (denoised, next_latents)
```

```python
import functools

import jax
import jax.numpy as jnp
from jax import lax
from jax.experimental import pallas as pl
from jax.experimental.pallas import tpu as pltpu
from jax.sharding import PartitionSpec as P

HDIM = 128
STEPS = 40


GUIDANCE = 3.5
flow_shift = 5.0


def from_partner(block, axis, bit):
    count = lax.axis_size(axis)
    route = []
    for low in range(count):
        high = low | 1 << bit
        if high != low and high < count:
            route += [(low, high), (high, low)]
    return lax.ppermute(block, axis, route)


def sigma_of(step):
    level = 1.0 - step.astype(jnp.float32) / STEPS
    return flow_shift * level / (1.0 + (flow_shift - 1.0) * level)


def combine(cond, uncond):
    base = uncond.astype(jnp.float32)
    return (base + GUIDANCE * (cond.astype(jnp.float32) - base)).astype(jnp.bfloat16)


def attend(stacked):
    query_heads, key_heads, value_heads = stacked
    items, length, width_dev = query_heads.shape
    heads_dev = width_dev // HDIM
    block = 512 if length % 512 == 0 else length
    key_rows = key_heads.reshape(items, length, heads_dev, HDIM)
    value_rows = value_heads.reshape(items, length, heads_dev, HDIM)
    query_blocks = query_heads.reshape(items, length // block, block, heads_dev, HDIM).transpose(
        1, 0, 2, 3, 4
    )

    def one_block(query_part):
        scores = jnp.einsum(
            "nqhd,nkhd->nhqk", query_part, key_rows, preferred_element_type=jnp.float32
        ) * HDIM ** (-0.5)
        weights = jax.nn.softmax(scores, axis=-1).astype(jnp.bfloat16)
        return jnp.einsum(
            "nhqk,nkhd->nqhd", weights, value_rows, preferred_element_type=jnp.float32
        ).astype(jnp.bfloat16)

    result = lax.map(one_block, query_blocks)
    return result.transpose(1, 0, 2, 3, 4).reshape(items, length, width_dev)


def exchange_heads(queries, keys, values, latents, gain, steps_table, flags):
    attended = attend(
        (
            lax.all_to_all(queries[0, 0], "seq", split_axis=2, concat_axis=1, tiled=True),
            lax.all_to_all(keys[0, 0], "seq", split_axis=2, concat_axis=1, tiled=True),
            lax.all_to_all(values[0, 0], "seq", split_axis=2, concat_axis=1, tiled=True),
        )
    )
    guided = lax.all_to_all(
        combine(attended[0], attended[1]), "seq", split_axis=0, concat_axis=1, tiled=True
    )
    guided_f32 = guided.astype(jnp.float32)
    scale = lax.rsqrt(jnp.mean(guided_f32 * guided_f32, axis=-1, keepdims=True) + 1e-06)
    velocity = guided_f32 * scale * gain[0].astype(jnp.float32)[None, :]
    step_now = steps_table[0, 0]
    sigma_now = sigma_of(step_now)
    sigma_next = sigma_of(step_now + 1)
    current = latents[0, 0].astype(jnp.float32)
    denoised = (current - sigma_now * velocity).astype(jnp.bfloat16)
    moved = (current + (sigma_next - sigma_now) * velocity).astype(jnp.bfloat16)
    partner = from_partner(moved, "expert", 0)
    next_latents = jnp.where(flags[0] == 1, partner, moved)
    return (denoised[None, None], next_latents[None, None])


MESH = pl.DeviceIdType.MESH
HEADS_AT_ONCE = 2
PIECE = 16


def head_cols(head):
    return pl.ds(pl.multiple_of(head * HDIM, HDIM), HDIM)


def partial_attention(query, key_rows, value_rows):
    scores = lax.dot_general(
        query, key_rows, (((1,), (1,)), ((), ())), preferred_element_type=jnp.float32
    )
    top = jnp.max(scores, axis=-1, keepdims=True)
    powers = jnp.exp((scores - top) * HDIM ** (-0.5))
    total = jnp.sum(powers, axis=-1, keepdims=True)
    part = jnp.dot(powers.astype(jnp.bfloat16), value_rows, preferred_element_type=jnp.float32)
    return part / total, top * HDIM ** (-0.5) + jnp.log(total)


def share(mine, other):
    return 1.0 / (1.0 + jnp.exp(other - mine))


def pair_kernel(
    queries, keys, values, latents, gain, steps,
    denoised, moved, partner,
    q_own, q_far, k_all, v_all, part_own, part_far, part_back, current, den_rows, mov_rows,
    guided, lse_own, lse_peer, lse_far, lse_back, gain_now, gain_move,
    load_sems, kv_sems, q_sems, lse_sems, back_sems, back_lse_sems, cross_sems, store_sems,
):
    seq = lax.axis_index("seq")
    size = lax.axis_size("seq")
    beside = {"seq": seq + 1 - 2 * lax.rem(seq, 2)}
    across = {"seq": lax.rem(seq + size // 2, size)}
    other = {"expert": 1 - lax.axis_index("expert")}
    branches, rows, width = queries.shape
    heads = width // HDIM
    half = rows // 2
    pieces = rows // PIECE

    own_keys = pl.ds(0, rows)
    loads = [
        pltpu.make_async_copy(queries, q_own, load_sems.at[0]),
        pltpu.make_async_copy(keys, k_all.at[:, own_keys], load_sems.at[1]),
        pltpu.make_async_copy(values, v_all.at[:, own_keys], load_sems.at[2]),
        pltpu.make_async_copy(latents, current, load_sems.at[3]),
    ]
    for load in loads:
        load.start()

    barrier = pltpu.get_barrier_semaphore()
    for peer in (beside, across, other):
        pl.semaphore_signal(barrier, inc=1, device_id=peer, device_id_type=MESH)
    pl.semaphore_wait(barrier, 3)

    def remote(source, target, sems, index, peer):
        return pltpu.make_async_remote_copy(
            src_ref=source, dst_ref=target, send_sem=sems.at[0, index],
            recv_sem=sems.at[1, index], device_id=peer, device_id_type=MESH,
        )

    q_sends = [
        remote(queries.at[:, pl.ds(at * half, half)], q_far.at[:, pl.ds(at * half, half)],
               q_sems, at, across)
        for at in range(2)
    ]
    q_sends[0].start()
    peer_keys = pl.ds(rows, rows)
    kv_sends = [
        remote(keys, k_all.at[:, peer_keys], kv_sems, 0, beside),
        remote(values, v_all.at[:, peer_keys], kv_sems, 1, beside),
    ]
    for send in kv_sends:
        send.start()

    step = jnp.full((1, HDIM), steps[0, 0], jnp.int32)
    sigma_now = sigma_of(step)[:, :1]
    sigma_next = sigma_of(step + 1)[:, :1]
    row = gain[...].astype(jnp.float32)
    gain_now[...] = sigma_now * row
    gain_move[...] = (sigma_next - sigma_now) * row

    for load in loads:
        load.wait()
    for send in kv_sends:
        send.wait_recv()

    lane = lax.broadcasted_iota(jnp.int32, (1, HDIM), 1)

    def own_heads(step_at, lse):
        for extra in range(HEADS_AT_ONCE):
            head = step_at * HEADS_AT_ONCE + extra
            cols = head_cols(head)
            for branch in range(branches):
                part, stat = partial_attention(
                    q_own[branch, :, cols], k_all[branch, :, cols], v_all[branch, :, cols]
                )
                part_own[branch, :, cols] = part
                lse = jnp.where(lane == branch * heads + head, stat, lse)
        return lse

    lse_own[...] = lax.fori_loop(
        0, heads // HEADS_AT_ONCE, own_heads, jnp.zeros((rows, HDIM), jnp.float32)
    )
    lse_send = remote(lse_own, lse_peer, lse_sems, 0, across)
    lse_send.start()
    q_sends[1].start()
    lse_send.wait_recv()

    def back_copies(piece):
        at = pl.ds(pl.multiple_of(piece * PIECE, PIECE), PIECE)
        return (
            remote(lse_far.at[at], lse_back.at[at], back_lse_sems, piece, across),
            remote(part_far.at[at], part_back.at[at], back_sems, piece, across),
        )

    for at in range(2):
        q_sends[at].wait_recv()
        here = pl.ds(at * half, half)
        peer_lse = lse_peer[here, :]

        def far_heads(step_at, lse):
            for extra in range(HEADS_AT_ONCE):
                head = step_at * HEADS_AT_ONCE + extra
                cols = head_cols(head)
                terms = []
                for branch in range(branches):
                    part, stat = partial_attention(
                        q_far[branch, here, cols], k_all[branch, :, cols], v_all[branch, :, cols]
                    )
                    spot = lane == branch * heads + head
                    lse = jnp.where(spot, stat, lse)
                    theirs = jnp.sum(jnp.where(spot, peer_lse, 0.0), axis=-1, keepdims=True)
                    terms.append(part * share(stat, theirs))
                part_far[here, cols] = (GUIDANCE * terms[0] + (1.0 - GUIDANCE) * terms[1]).astype(
                    jnp.bfloat16
                )
            return lse

        lse_far[here, :] = lax.fori_loop(
            0, heads // HEADS_AT_ONCE, far_heads, jnp.zeros((half, HDIM), jnp.float32)
        )
        for piece in range(at * pieces // 2, (at + 1) * pieces // 2):
            for copy in back_copies(piece):
                copy.start()

    def result_copies(piece):
        at = pl.ds(pl.multiple_of(piece * PIECE, PIECE), PIECE)
        return (
            remote(mov_rows.at[at], partner.at[at], cross_sems, piece, other),
            pltpu.make_async_copy(den_rows.at[at], denoised.at[at], store_sems.at[0, piece]),
            pltpu.make_async_copy(mov_rows.at[at], moved.at[at], store_sems.at[1, piece]),
        )

    def finish(piece, carry):
        at = pl.ds(pl.multiple_of(piece * PIECE, PIECE), PIECE)
        for copy in back_copies(piece):
            copy.wait_recv()
        weight = share(lse_own[at, :], lse_back[at, :])
        squares = jnp.zeros((PIECE, HDIM), jnp.float32)
        for head in range(heads):
            cols = pl.ds(head * HDIM, HDIM)
            uncond = heads + head
            value = (
                GUIDANCE * weight[:, head : head + 1] * part_own[0, at, cols]
                + (1.0 - GUIDANCE) * weight[:, uncond : uncond + 1] * part_own[1, at, cols]
                + part_back[at, cols].astype(jnp.float32)
            ).astype(jnp.bfloat16).astype(jnp.float32)
            guided[:, cols] = value
            squares += value * value
        mean = jnp.sum(squares, axis=-1, keepdims=True) / width
        scale = lax.rsqrt(mean + 1e-06)
        for head in range(heads):
            cols = pl.ds(head * HDIM, HDIM)
            unit = guided[:, cols] * scale
            now = current[at, cols].astype(jnp.float32)
            mov_rows[at, cols] = (now + gain_move[:, cols] * unit).astype(jnp.bfloat16)
            den_rows[at, cols] = (now - gain_now[:, cols] * unit).astype(jnp.bfloat16)
        for copy in result_copies(piece):
            copy.start()
        return carry

    lax.fori_loop(0, pieces, finish, 0)

    for send in q_sends + kv_sends + [lse_send]:
        send.wait_send()

    def drain(piece, carry):
        for copy in back_copies(piece):
            copy.wait_send()
        for copy in result_copies(piece):
            copy.wait()
        return carry

    lax.fori_loop(0, pieces, drain, 0)


def exchange_queries(queries, keys, values, latents, gain, steps_table, flags):
    branches, rows, width = queries.shape[2:]
    pieces = rows // PIECE
    whole = jax.ShapeDtypeStruct((rows, width), jnp.bfloat16)
    hbm = pl.BlockSpec(memory_space=pltpu.HBM)
    low = functools.partial(pltpu.VMEM, dtype=jnp.bfloat16)
    high = functools.partial(pltpu.VMEM, dtype=jnp.float32)
    dma = pltpu.SemaphoreType.DMA
    denoised, moved, partner = pl.pallas_call(
        pair_kernel,
        out_shape=(whole, whole, whole),
        in_specs=[hbm] * 4
        + [pl.BlockSpec(memory_space=pltpu.VMEM), pl.BlockSpec(memory_space=pltpu.SMEM)],
        out_specs=(hbm, hbm, hbm),
        scratch_shapes=[
            low((branches, rows, width)),
            low((branches, rows, width)),
            low((branches, 2 * rows, width)),
            low((branches, 2 * rows, width)),
            high((branches, rows, width)),
            low((rows, width)),
            low((rows, width)),
            low((rows, width)),
            low((rows, width)),
            low((rows, width)),
            high((PIECE, width)),
            high((rows, HDIM)),
            high((rows, HDIM)),
            high((rows, HDIM)),
            high((rows, HDIM)),
            high((1, width)),
            high((1, width)),
            dma((4,)),
            dma((2, 2)),
            dma((2, 2)),
            dma((2, 1)),
            dma((2, pieces)),
            dma((2, pieces)),
            dma((2, pieces)),
            dma((2, pieces)),
        ],
        compiler_params=pltpu.CompilerParams(collective_id=0, has_side_effects=True),
    )(queries[0, 0], keys[0, 0], values[0, 0], latents[0, 0], gain, steps_table)
    next_latents = jnp.where(flags[0] == 1, partner, moved)
    return (denoised[None, None], next_latents[None, None])


def per_device(*blocks):
    branches, rows, width = blocks[0].shape[2:]
    paired = (
        lax.axis_size("seq") == 2 * 2
        and lax.axis_size("expert") == 2
        and rows % (2 * PIECE) == 0
        and branches * width // HDIM <= HDIM
    )
    return (exchange_queries if paired else exchange_heads)(*blocks)


def solution(mesh):
    placed = (
        P("expert", "batch", None, "seq", None),
        P("expert", "batch", None, "seq", None),
        P("expert", "batch", None, "seq", None),
        P("expert", "batch", "seq", None),
        P("expert", None),
        P("expert", "batch"),
        P("batch"),
    )
    return jax.shard_map(
        per_device,
        mesh=mesh,
        in_specs=placed,
        out_specs=(P("expert", "batch", "seq", None), P("expert", "batch", "seq", None)),
        check_vma=False,
    )
```

```python
import functools

import jax
import jax.numpy as jnp
from jax import lax
from jax.experimental import pallas as pl
from jax.experimental.pallas import tpu as pltpu
from jax.sharding import PartitionSpec as P

HDIM = 128
STEPS = 40


GUIDANCE = 3.5
flow_shift = 5.0


def from_partner(block, axis, bit):
    count = lax.axis_size(axis)
    route = []
    for low in range(count):
        high = low | 1 << bit
        if high != low and high < count:
            route += [(low, high), (high, low)]
    return lax.ppermute(block, axis, route)


def sigma_of(step):
    level = 1.0 - step.astype(jnp.float32) / STEPS
    return flow_shift * level / (1.0 + (flow_shift - 1.0) * level)


def combine(cond, uncond):
    base = uncond.astype(jnp.float32)
    return (base + GUIDANCE * (cond.astype(jnp.float32) - base)).astype(jnp.bfloat16)


def attend(stacked):
    query_heads, key_heads, value_heads = stacked
    items, length, width_dev = query_heads.shape
    heads_dev = width_dev // HDIM
    block = 512 if length % 512 == 0 else length
    key_rows = key_heads.reshape(items, length, heads_dev, HDIM)
    value_rows = value_heads.reshape(items, length, heads_dev, HDIM)
    query_blocks = query_heads.reshape(items, length // block, block, heads_dev, HDIM).transpose(
        1, 0, 2, 3, 4
    )

    def one_block(query_part):
        scores = jnp.einsum(
            "nqhd,nkhd->nhqk", query_part, key_rows, preferred_element_type=jnp.float32
        ) * HDIM ** (-0.5)
        weights = jax.nn.softmax(scores, axis=-1).astype(jnp.bfloat16)
        return jnp.einsum(
            "nhqk,nkhd->nqhd", weights, value_rows, preferred_element_type=jnp.float32
        ).astype(jnp.bfloat16)

    result = lax.map(one_block, query_blocks)
    return result.transpose(1, 0, 2, 3, 4).reshape(items, length, width_dev)


def exchange_heads(queries, keys, values, latents, gain, steps_table, flags):
    attended = attend(
        (
            lax.all_to_all(queries[0, 0], "seq", split_axis=2, concat_axis=1, tiled=True),
            lax.all_to_all(keys[0, 0], "seq", split_axis=2, concat_axis=1, tiled=True),
            lax.all_to_all(values[0, 0], "seq", split_axis=2, concat_axis=1, tiled=True),
        )
    )
    guided = lax.all_to_all(
        combine(attended[0], attended[1]), "seq", split_axis=0, concat_axis=1, tiled=True
    )
    guided_f32 = guided.astype(jnp.float32)
    scale = lax.rsqrt(jnp.mean(guided_f32 * guided_f32, axis=-1, keepdims=True) + 1e-06)
    velocity = guided_f32 * scale * gain[0].astype(jnp.float32)[None, :]
    step_now = steps_table[0, 0]
    sigma_now = sigma_of(step_now)
    sigma_next = sigma_of(step_now + 1)
    current = latents[0, 0].astype(jnp.float32)
    denoised = (current - sigma_now * velocity).astype(jnp.bfloat16)
    moved = (current + (sigma_next - sigma_now) * velocity).astype(jnp.bfloat16)
    partner = from_partner(moved, "expert", 0)
    next_latents = jnp.where(flags[0] == 1, partner, moved)
    return (denoised[None, None], next_latents[None, None])


MESH = pl.DeviceIdType.MESH
HEADS_AT_ONCE = 4
PIECE = 16
LATE = 2


def head_cols(head):
    return pl.ds(pl.multiple_of(head * HDIM, HDIM), HDIM)


def partial_attention(query, key_rows, value_rows):
    scores = lax.dot_general(
        query, key_rows, (((1,), (1,)), ((), ())), preferred_element_type=jnp.float32
    )
    top = jnp.max(scores, axis=-1, keepdims=True)
    powers = jnp.exp((scores - top) * HDIM ** (-0.5))
    total = jnp.sum(powers, axis=-1, keepdims=True)
    part = jnp.dot(powers.astype(jnp.bfloat16), value_rows, preferred_element_type=jnp.float32)
    return part / total, top * HDIM ** (-0.5) + jnp.log(total)


def share(mine, other):
    return 1.0 / (1.0 + jnp.exp(other - mine))


def pair_kernel(
    queries, keys, values, latents, gain, steps,
    denoised, moved, partner,
    q_own, q_far, k_all, v_all, part_own, part_far, part_back, current, den_rows, mov_rows,
    guided, lse_own, lse_peer, lse_far, lse_back, gain_now, gain_move,
    load_sems, kv_sems, q_sems, lse_sems, back_sems, back_lse_sems, cross_sems, store_sems,
):
    seq = lax.axis_index("seq")
    size = lax.axis_size("seq")
    beside = {"seq": seq + 1 - 2 * lax.rem(seq, 2)}
    across = {"seq": lax.rem(seq + size // 2, size)}
    other = {"expert": 1 - lax.axis_index("expert")}
    branches, rows, width = queries.shape
    heads = width // HDIM
    half = rows // 2
    pieces = rows // PIECE

    own_keys = pl.ds(0, rows)
    loads = [
        pltpu.make_async_copy(queries, q_own, load_sems.at[0]),
        pltpu.make_async_copy(keys, k_all.at[:, own_keys], load_sems.at[1]),
        pltpu.make_async_copy(values, v_all.at[:, own_keys], load_sems.at[2]),
        pltpu.make_async_copy(latents, current, load_sems.at[3]),
    ]
    for load in loads:
        load.start()

    barrier = pltpu.get_barrier_semaphore()
    for peer in (beside, across, other):
        pl.semaphore_signal(barrier, inc=1, device_id=peer, device_id_type=MESH)
    pl.semaphore_wait(barrier, 3)

    def remote(source, target, sems, index, peer):
        return pltpu.make_async_remote_copy(
            src_ref=source, dst_ref=target, send_sem=sems.at[0, index],
            recv_sem=sems.at[1, index], device_id=peer, device_id_type=MESH,
        )

    q_sends = [
        remote(queries.at[:, pl.ds(at * PIECE, PIECE)], q_far.at[:, pl.ds(at * PIECE, PIECE)],
               q_sems, at, across)
        for at in range(pieces)
    ]
    peer_keys = pl.ds(rows, rows)
    kv_sends = [
        remote(keys, k_all.at[:, peer_keys], kv_sems, 0, beside),
        remote(values, v_all.at[:, peer_keys], kv_sems, 1, beside),
    ]
    for send in kv_sends:
        send.start()
    for send in q_sends[:-LATE]:
        send.start()

    step = jnp.full((1, HDIM), steps[0, 0], jnp.int32)
    sigma_now = sigma_of(step)[:, :1]
    sigma_next = sigma_of(step + 1)[:, :1]
    row = gain[...].astype(jnp.float32)
    gain_now[...] = sigma_now * row
    gain_move[...] = (sigma_next - sigma_now) * row

    for load in loads:
        load.wait()
    for send in kv_sends:
        send.wait_recv()

    lane = lax.broadcasted_iota(jnp.int32, (1, HDIM), 1)

    def own_heads(step_at, lse):
        for extra in range(HEADS_AT_ONCE):
            head = step_at * HEADS_AT_ONCE + extra
            cols = head_cols(head)
            for branch in range(branches):
                part, stat = partial_attention(
                    q_own[branch, :, cols], k_all[branch, :, cols], v_all[branch, :, cols]
                )
                part_own[branch, :, cols] = part
                lse = jnp.where(lane == branch * heads + head, stat, lse)
        return lse

    lse_own[...] = lax.fori_loop(
        0, heads // HEADS_AT_ONCE, own_heads, jnp.zeros((rows, HDIM), jnp.float32)
    )
    lse_send = remote(lse_own, lse_peer, lse_sems, 0, across)
    lse_send.start()
    for send in q_sends[-LATE:]:
        send.start()
    lse_send.wait_recv()

    def back_copies(piece):
        at = pl.ds(pl.multiple_of(piece * PIECE, PIECE), PIECE)
        return (
            remote(lse_far.at[at], lse_back.at[at], back_lse_sems, piece, across),
            remote(part_far.at[at], part_back.at[at], back_sems, piece, across),
        )

    for at in range(2):
        for send in q_sends[at * pieces // 2 : (at + 1) * pieces // 2]:
            send.wait_recv()
        here = pl.ds(at * half, half)
        peer_lse = lse_peer[here, :]

        def far_heads(step_at, lse):
            for extra in range(HEADS_AT_ONCE):
                head = step_at * HEADS_AT_ONCE + extra
                cols = head_cols(head)
                terms = []
                for branch in range(branches):
                    part, stat = partial_attention(
                        q_far[branch, here, cols], k_all[branch, :, cols], v_all[branch, :, cols]
                    )
                    spot = lane == branch * heads + head
                    lse = jnp.where(spot, stat, lse)
                    theirs = jnp.sum(jnp.where(spot, peer_lse, 0.0), axis=-1, keepdims=True)
                    terms.append(part * share(stat, theirs))
                part_far[here, cols] = (GUIDANCE * terms[0] + (1.0 - GUIDANCE) * terms[1]).astype(
                    jnp.bfloat16
                )
            return lse

        lse_far[here, :] = lax.fori_loop(
            0, heads // HEADS_AT_ONCE, far_heads, jnp.zeros((half, HDIM), jnp.float32)
        )
        for piece in range(at * pieces // 2, (at + 1) * pieces // 2):
            for copy in back_copies(piece):
                copy.start()

    def result_copies(piece):
        at = pl.ds(pl.multiple_of(piece * PIECE, PIECE), PIECE)
        return (
            remote(mov_rows.at[at], partner.at[at], cross_sems, piece, other),
            pltpu.make_async_copy(den_rows.at[at], denoised.at[at], store_sems.at[0, piece]),
            pltpu.make_async_copy(mov_rows.at[at], moved.at[at], store_sems.at[1, piece]),
        )

    def finish(piece, carry):
        at = pl.ds(pl.multiple_of(piece * PIECE, PIECE), PIECE)
        for copy in back_copies(piece):
            copy.wait_recv()
        weight = share(lse_own[at, :], lse_back[at, :])
        squares = jnp.zeros((PIECE, HDIM), jnp.float32)
        for head in range(heads):
            cols = pl.ds(head * HDIM, HDIM)
            uncond = heads + head
            value = (
                GUIDANCE * weight[:, head : head + 1] * part_own[0, at, cols]
                + (1.0 - GUIDANCE) * weight[:, uncond : uncond + 1] * part_own[1, at, cols]
                + part_back[at, cols].astype(jnp.float32)
            ).astype(jnp.bfloat16).astype(jnp.float32)
            guided[:, cols] = value
            squares += value * value
        mean = jnp.sum(squares, axis=-1, keepdims=True) / width
        scale = lax.rsqrt(mean + 1e-06)
        for head in range(heads):
            cols = pl.ds(head * HDIM, HDIM)
            unit = guided[:, cols] * scale
            now = current[at, cols].astype(jnp.float32)
            mov_rows[at, cols] = (now + gain_move[:, cols] * unit).astype(jnp.bfloat16)
            den_rows[at, cols] = (now - gain_now[:, cols] * unit).astype(jnp.bfloat16)
        for copy in result_copies(piece):
            copy.start()
        return carry

    lax.fori_loop(0, pieces, finish, 0)

    for send in q_sends + kv_sends + [lse_send]:
        send.wait_send()

    def drain(piece, carry):
        for copy in back_copies(piece):
            copy.wait_send()
        for copy in result_copies(piece):
            copy.wait()
        return carry

    lax.fori_loop(0, pieces, drain, 0)


def exchange_queries(queries, keys, values, latents, gain, steps_table, flags):
    branches, rows, width = queries.shape[2:]
    pieces = rows // PIECE
    whole = jax.ShapeDtypeStruct((rows, width), jnp.bfloat16)
    hbm = pl.BlockSpec(memory_space=pltpu.HBM)
    low = functools.partial(pltpu.VMEM, dtype=jnp.bfloat16)
    high = functools.partial(pltpu.VMEM, dtype=jnp.float32)
    dma = pltpu.SemaphoreType.DMA
    denoised, moved, partner = pl.pallas_call(
        pair_kernel,
        out_shape=(whole, whole, whole),
        in_specs=[hbm] * 4
        + [pl.BlockSpec(memory_space=pltpu.VMEM), pl.BlockSpec(memory_space=pltpu.SMEM)],
        out_specs=(hbm, hbm, hbm),
        scratch_shapes=[
            low((branches, rows, width)),
            low((branches, rows, width)),
            low((branches, 2 * rows, width)),
            low((branches, 2 * rows, width)),
            high((branches, rows, width)),
            low((rows, width)),
            low((rows, width)),
            low((rows, width)),
            low((rows, width)),
            low((rows, width)),
            high((PIECE, width)),
            high((rows, HDIM)),
            high((rows, HDIM)),
            high((rows, HDIM)),
            high((rows, HDIM)),
            high((1, width)),
            high((1, width)),
            dma((4,)),
            dma((2, 2)),
            dma((2, pieces)),
            dma((2, 1)),
            dma((2, pieces)),
            dma((2, pieces)),
            dma((2, pieces)),
            dma((2, pieces)),
        ],
        compiler_params=pltpu.CompilerParams(collective_id=0, has_side_effects=True),
    )(queries[0, 0], keys[0, 0], values[0, 0], latents[0, 0], gain, steps_table)
    next_latents = jnp.where(flags[0] == 1, partner, moved)
    return (denoised[None, None], next_latents[None, None])


def per_device(*blocks):
    branches, rows, width = blocks[0].shape[2:]
    paired = (
        lax.axis_size("seq") == 2 * 2
        and lax.axis_size("expert") == 2
        and rows % (2 * PIECE) == 0
        and branches * width // HDIM <= HDIM
    )
    return (exchange_queries if paired else exchange_heads)(*blocks)


def solution(mesh):
    placed = (
        P("expert", "batch", None, "seq", None),
        P("expert", "batch", None, "seq", None),
        P("expert", "batch", None, "seq", None),
        P("expert", "batch", "seq", None),
        P("expert", None),
        P("expert", "batch"),
        P("batch"),
    )
    return jax.shard_map(
        per_device,
        mesh=mesh,
        in_specs=placed,
        out_specs=(P("expert", "batch", "seq", None), P("expert", "batch", "seq", None)),
        check_vma=False,
    )
```
